32 devices in a mesh: dp: 16 (over z, y, core), tensor: 2 (over x).
Axes of the slice: x: 2, y: 2, z: 4, core: 2. Of those that a mesh axis runs over, the one named last changes fastest.
Arguments:
- step: int32 [1], replicated, may hold values from 0 to 999
- activations: bfloat16 [2, 16384, 8192], P(None, 'dp', 'tensor'), may hold values from -6 to 6
- grad_weight: bfloat16 [2, 8192, 28672], P(None, 'tensor', 'dp'), may hold values from -6 to 6
Outputs:
- preconditioned: float32 [8192, 28672], P('tensor', 'dp')
The draws below stay inside these ranges and needn't reach their ends.
All inputs are finite; a program needn't handle non-finite values.
Results may differ from the reference program's by a relative error of at most 0.0044.
Values may be sent and summed in bfloat16 or wider, within the bound.
No kernel may reach another device: no remote copies, remote signals or barrier semaphores. Data moves between devices by JAX's collectives and lax.ppermute only.
A program may use at most 192 MiB of HBM per device.

```python
import jax
import jax.numpy as jnp
from jax import lax

D = 8192
FF = 28672
BLOCK = 1024
LAYERS = 2
ITERS = 4
TOKENS = 16384


def block_scale(stream_key, extent, shards, smallest, high):
    loudness, own = 1.0, jax.random.fold_in(stream_key, 6)
    for dim, parts in shards:
        draws = jnp.exp(jax.random.uniform(jax.random.fold_in(own, dim), (parts,), jnp.float32, smallest / len(shards), high / len(shards)))
        loudness = loudness * jnp.repeat(draws, extent[dim] // parts).reshape([-1 if axis == dim else 1 for axis in range(len(extent))])
    return loudness


def scatter_about(stream_key, shape, scale, limit, split=(), held_as=jnp.bfloat16):
    values = jax.random.normal(stream_key, shape, jnp.float32) * scale
    if len(split) > 0:
        values = block_scale(stream_key, shape, split, -0.22, 0.18) * values
    return jnp.clip(values, min=-limit, max=limit).astype(held_as)


def setup_inputs(seed: int = 0) -> dict:
    arg_keys = jax.random.split(jax.random.key(seed), 4)
    step = jax.random.randint(arg_keys[0], (1,), 0, 1000).astype(jnp.int32)
    activations = scatter_about(arg_keys[1], (LAYERS, TOKENS, D), 1.0, 6.0, ((1, 16), (2, 2)))
    grad_weight = scatter_about(arg_keys[2], (LAYERS, D, FF), 1.0, 6.0, ((1, 2), (2, 16)))
    return {"step": step, "activations": activations, "grad_weight": grad_weight}


def reference(step, activations, grad_weight):
    layer = step[0] % LAYERS
    damping = 0.05 + 0.1 * step[0].astype(jnp.float32) / 1000.0
    acts = lax.dynamic_index_in_dim(activations, layer, 0, keepdims=False)
    grads = lax.dynamic_index_in_dim(grad_weight, layer, 0, keepdims=False)
    count = D // BLOCK
    identity = jnp.eye(BLOCK, dtype=jnp.float32)
    indices = jnp.arange(count, dtype=jnp.int32)

    def gram_of(index):
        cols = lax.dynamic_slice_in_dim(acts, index * BLOCK, BLOCK, 1)
        gram = jnp.dot(cols.T, cols, preferred_element_type=jnp.float32)
        return gram / TOKENS + damping * identity
    factors = lax.map(gram_of, indices)
    largest = jnp.max(lax.optimization_barrier(jnp.sum(factors * factors, axis=(1, 2))))

    def invert(pair):
        factor, index = pair
        iterate = identity / jnp.sqrt(largest)
        for sweep in range(ITERS):
            product = jnp.dot(factor, iterate, precision=lax.Precision.HIGHEST)
            iterate = 2.0 * iterate - jnp.dot(product, iterate, precision=lax.Precision.HIGHEST)
        inverse = iterate.astype(jnp.bfloat16)
        rows = lax.dynamic_slice_in_dim(grads, index * BLOCK, BLOCK, 0)
        return jnp.dot(inverse, rows, preferred_element_type=jnp.float32)
    result = lax.map(invert, (factors, indices))
    return result.reshape(D, FF)
```

```python
import jax
import jax.numpy as jnp
from jax import lax
from jax.experimental import pallas as pl
from jax.experimental.pallas import tpu as pltpu
from jax.sharding import PartitionSpec as P


BLOCK = 1024
LAYERS = 2
TILE = 256
HALF = TILE // 2
NT = BLOCK // TILE
OFF = [(i, j) for i in range(NT) for j in range(i + 1, NT)]
SLOTS = len(OFF) + NT - 1
ROWS = SLOTS * TILE
QUARTS = ((0, 0), (0, HALF), (HALF, HALF))
DIAG0 = len(OFF)
LIMIT = 60 * 1024 * 1024


def pack(dst, tile_of):
    for s, (i, j) in enumerate(OFF):
        dst[s * TILE:(s + 1) * TILE, :] = tile_of(i, j).astype(dst.dtype)
    last = tile_of(NT - 1, NT - 1).astype(dst.dtype)
    for d in range(NT - 1):
        r = (DIAG0 + d) * TILE
        t = tile_of(d, d).astype(dst.dtype)
        dst[r:r + HALF, :] = t[:HALF, :]
        dst[r + HALF:r + TILE, HALF:] = t[HALF:, HALF:]
        y, x = QUARTS[d]
        dst[r + HALF:r + TILE, :HALF] = last[y:y + HALF, x:x + HALF]


def unpack(src, put, dtype):
    for s, (i, j) in enumerate(OFF):
        t = src[s * TILE:(s + 1) * TILE, :].astype(dtype)
        put(i * TILE, j * TILE, t)
        put(j * TILE, i * TILE, t.T)
    for d in range(NT - 1):
        r = (DIAG0 + d) * TILE
        o = d * TILE
        upper = src[r:r + HALF, HALF:].astype(dtype)
        put(o, o, src[r:r + HALF, :HALF].astype(dtype))
        put(o, o + HALF, upper)
        put(o + HALF, o, upper.T)
        put(o + HALF, o + HALF, src[r + HALF:r + TILE, HALF:].astype(dtype))
        y, x = QUARTS[d]
        e = (NT - 1) * TILE
        part = src[r + HALF:r + TILE, :HALF].astype(dtype)
        put(e + y, e + x, part)
        if x != y:
            put(e + x, e + y, part.T)


def dot(a, b, dims=((1,), (0,))):
    return lax.dot_general(a, b, (dims, ((), ())), preferred_element_type=jnp.float32)


def gram_body(info, acts, keep, send, scratch):
    for i in range(NT):
        panel = dot(acts[:, i * TILE:(i + 1) * TILE], acts[:, i * TILE:], ((0,), (0,)))
        for s, (a, b) in enumerate(OFF):
            if a == i:
                o = (b - i) * TILE
                scratch[s * TILE:(s + 1) * TILE, :] = panel[:, o:o + TILE].astype(scratch.dtype)
        t = panel[:, :TILE].astype(scratch.dtype)
        if i < NT - 1:
            r = (DIAG0 + i) * TILE
            scratch[r:r + HALF, :] = t[:HALF, :]
            scratch[r + HALF:r + TILE, HALF:] = t[HALF:, HALF:]
        else:
            for d, (y, x) in enumerate(QUARTS):
                r = (DIAG0 + d) * TILE
                scratch[r + HALF:r + TILE, :HALF] = t[y:y + HALF, x:x + HALF]
    if send is None:
        keep[...] = scratch[...]
    else:
        rows = ROWS // 2
        core = info[1]
        keep[...] = scratch[pl.ds(pl.multiple_of(core * rows, HALF), rows), :]
        send[...] = scratch[pl.ds(pl.multiple_of((1 - core) * rows, HALF), rows), :]


def gram(info, activations, nblock, split):
    tok = activations.shape[1]
    rows = ROWS // 2 if split else ROWS
    spec = pl.BlockSpec((None, rows, TILE), lambda b, info: (b, 0, 0))
    shape = jax.ShapeDtypeStruct((nblock, rows, TILE), jnp.bfloat16)

    def body(info, acts, *rest):
        if split:
            gram_body(info, acts, *rest)
        else:
            gram_body(info, acts, rest[0], None, rest[1])

    return pl.pallas_call(
        body,
        grid_spec=pltpu.PrefetchScalarGridSpec(
            num_scalar_prefetch=1,
            grid=(nblock,),
            in_specs=[pl.BlockSpec((None, tok, BLOCK), lambda b, info: (info[0], 0, b))],
            out_specs=[spec, spec] if split else [spec],
            scratch_shapes=[pltpu.VMEM((ROWS, TILE), jnp.bfloat16)],
        ),
        out_shape=[shape, shape] if split else [shape],
        compiler_params=pltpu.CompilerParams(vmem_limit_bytes=LIMIT),
        name="gram",
    )(info, activations)


def squares(packed, damping, tokens):
    f = packed.astype(jnp.float32)
    r = lax.broadcasted_iota(jnp.int32, (ROWS, TILE), 0)
    c = lax.broadcasted_iota(jnp.int32, (ROWS, TILE), 1)
    slot = r // TILE - DIAG0
    rr = r % TILE
    low = (rr >= HALF) & (c < HALF)
    on = ((low & (rr - HALF == c) & (slot != 1)) | (rr == c)) & (slot >= 0)
    twice = (slot < 0) | (low & (slot == 1)) | ((rr < HALF) & (c >= HALF))
    f = f / tokens + jnp.where(on, damping, 0.0)
    return jnp.sum(f * f * jnp.where(twice, 2.0, 1.0))


def factor_into(damp, packed, f, fb, tokens):
    damping = damp[0]
    inv = 1.0 / tokens

    def put(r, c, v):
        h, w = v.shape
        v = v * inv
        if r == c:
            eye = (lax.broadcasted_iota(jnp.int32, v.shape, 0)
                   == lax.broadcasted_iota(jnp.int32, v.shape, 1))
            v = v + jnp.where(eye, damping, 0.0)
        if f is not None:
            f[r:r + h, c:c + w] = v
        if fb is not None:
            fb[r:r + h, c:c + w] = v.astype(jnp.bfloat16)

    unpack(packed, put, jnp.float32)


STRIPS = [slice(i * TILE, (i + 1) * TILE) for i in range(NT)]


VM = pl.BlockSpec(memory_space=pltpu.VMEM)
SM = pl.BlockSpec(memory_space=pltpu.SMEM)
THIN = jax.ShapeDtypeStruct((BLOCK, BLOCK), jnp.bfloat16)
PARAMS = pltpu.CompilerParams(vmem_limit_bytes=LIMIT)


ANY = pl.BlockSpec(memory_space=pl.ANY)
VFULL = pltpu.VMEM((BLOCK, BLOCK), jnp.float32)
VTHIN = pltpu.VMEM((BLOCK, BLOCK), jnp.bfloat16)


def powers_body(damp, packed, h2, h3, fb, p2, p3, sems, *, tokens):
    factor_into(damp, packed, None, fb, tokens)
    for r in STRIPS:
        p2[r, :] = dot(fb[r, :], fb[...]).astype(p2.dtype)
    first = pltpu.make_async_copy(p2, h2, sems.at[0])
    first.start()
    for r in STRIPS:
        p3[r, :] = dot(p2[r, :], fb[...]).astype(p3.dtype)
    second = pltpu.make_async_copy(p3, h3, sems.at[1])
    second.start()
    first.wait()
    second.wait()


def powers(damping, packed, tokens):
    return pl.pallas_call(
        lambda *refs: powers_body(*refs, tokens=tokens),
        in_specs=[SM, VM],
        out_specs=[ANY, ANY],
        out_shape=[THIN, THIN],
        scratch_shapes=[VTHIN, VTHIN, VTHIN, pltpu.SemaphoreType.DMA((2,))],
        compiler_params=PARAMS,
        cost_estimate=pl.CostEstimate(
            flops=4 * BLOCK**3, transcendentals=0, bytes_accessed=BLOCK * BLOCK * 6
        ),
        name="powers",
    )(damping, packed)


def finish_body(info, damp, top, packed, h2, h3, out, piece, f, p2, p3, e, h, k, eb, kb, sems, *, tokens):
    loads = [pltpu.make_async_copy(a, b, sems.at[i]) for i, (a, b) in enumerate(((h2, p2), (h3, p3)))]
    for load in loads:
        load.start()
    factor_into(damp, packed, f, None, tokens)
    c = 1.0 / jnp.sqrt(jnp.max(top[...], axis=(0, 1), keepdims=True))
    for load in loads:
        load.wait()
    for r in STRIPS:
        cf = c * f[r, :]
        q2 = (c * c) * p2[r, :].astype(jnp.float32)
        q3 = (c * c * c) * p3[r, :].astype(jnp.float32)
        v = 3.0 * (cf - q2) + q3
        e[r, :] = v
        eb[r, :] = v.astype(jnp.bfloat16)
        f[r, :] = 6.0 * cf - 4.0 * q2 + q3
    for r in STRIPS:
        hv = 2.0 * e[r, :] - dot(eb[r, :], eb[...])
        h[r, :] = hv
        w = hv + 0.5 * e[r, :]
        kb[r, :] = w.astype(jnp.bfloat16)
    for r in STRIPS:
        k[r, :] = 3.75 * h[r, :] + 2.5 * e[r, :] - dot(kb[r, :], kb[...])
    for r in STRIPS:
        kb[r, :] = k[r, :].astype(jnp.bfloat16)
    for i, r in enumerate(STRIPS):
        cols = slice(i * TILE, BLOCK)
        x = dot(f[r, :].astype(jnp.bfloat16), kb[:, cols]) - 3.0 * k[r, cols] - 5.0 * f[r, cols]
        eye = (lax.broadcasted_iota(jnp.int32, x.shape, 0)
               == lax.broadcasted_iota(jnp.int32, x.shape, 1))
        e[r, cols] = c * (x + jnp.where(eye, 16.0, 0.0))
    pack(out, lambda i, j: e[i * TILE:(i + 1) * TILE, j * TILE:(j + 1) * TILE])
    n = piece.shape[0]
    piece[...] = out[pl.ds(pl.multiple_of(info[8] * n, HALF // 2), n), :]


def finish(info, damping, top, packed, p2, p3, tokens):
    return pl.pallas_call(
        lambda *refs: finish_body(*refs, tokens=tokens),
        in_specs=[SM, SM, VM, VM, ANY, ANY],
        out_specs=[VM, VM],
        out_shape=[
            jax.ShapeDtypeStruct((ROWS, TILE), jnp.bfloat16),
            jax.ShapeDtypeStruct((ROWS // 4, TILE), jnp.bfloat16),
        ],
        scratch_shapes=[VFULL, VTHIN, VTHIN, VFULL, VFULL, VFULL, VTHIN, VTHIN,
                        pltpu.SemaphoreType.DMA((2,))],
        compiler_params=PARAMS,
        name="finish",
    )(info, damping, top, packed, p2, p3)


CHUNK = 512
DEPTH = 3


def apply_body(info, *refs, count, blocks, first, aliased, cols):
    npiece = count * len(blocks)
    pieces = refs[:npiece]
    grads = refs[npiece]
    out, packed, x, g, o, psem, gsem, osem = refs[npiece + 1 + aliased:]
    n = ROWS // count
    chunks = [(c, min(CHUNK, cols - c)) for c in range(0, cols, CHUNK)]
    steps = [(b, c, w) for b in range(len(blocks)) for c, w in chunks]

    def rows(b):
        return pl.ds(pl.multiple_of(info[blocks[b]] * BLOCK, BLOCK), BLOCK)

    def load(s):
        b, c, w = steps[s]
        return pltpu.make_async_copy(
            grads.at[info[0], rows(b), pl.ds(c, w)], g.at[s % DEPTH, :, pl.ds(0, w)], gsem.at[s % DEPTH])

    def store(s):
        b, c, w = steps[s]
        return pltpu.make_async_copy(
            o.at[s % DEPTH, :, pl.ds(0, w)], out.at[rows(b), pl.ds(c, w)], osem.at[s % DEPTH])

    def fetch(b, p):
        start = pl.multiple_of(info[first + p] * n, HALF // 2)
        return pltpu.make_async_copy(
            pieces[b * count + p], packed.at[b, pl.ds(start, n), :], psem.at[b * count + p])

    for b in range(len(blocks)):
        for p in range(count):
            fetch(b, p).start()
    for s in range(min(DEPTH, len(steps))):
        load(s).start()
    for s, (b, c, w) in enumerate(steps):
        if c == 0:
            for p in range(count):
                fetch(b, p).wait()

            def put(r, col, v):
                x[b % 2, r:r + v.shape[0], col:col + v.shape[1]] = v

            unpack(packed.at[b], put, x.dtype)
        load(s).wait()
        if s >= DEPTH:
            store(s - DEPTH).wait()
        for r in STRIPS:
            o[s % DEPTH, r, :w] = dot(x[b % 2, r, :], g[s % DEPTH, :, :w])
        store(s).start()
        if s + DEPTH < len(steps):
            load(s + DEPTH).start()
    for s in range(max(0, len(steps) - DEPTH), len(steps)):
        store(s).wait()


def apply_blocks(info, blocks, first, pieces, grad_weight, result):
    width, cols = grad_weight.shape[1:]
    count = len(pieces) // len(blocks)
    aliased = result is not None
    return pl.pallas_call(
        lambda *refs: apply_body(
            *refs, count=count, blocks=blocks, first=first, aliased=int(aliased), cols=cols),
        in_specs=[SM] + [ANY] * (len(pieces) + 1 + int(aliased)),
        out_specs=ANY,
        scratch_shapes=[
            pltpu.VMEM((len(blocks), ROWS, TILE), jnp.bfloat16),
            pltpu.VMEM((2, BLOCK, BLOCK), jnp.bfloat16),
            pltpu.VMEM((DEPTH, BLOCK, CHUNK), jnp.bfloat16),
            pltpu.VMEM((DEPTH, BLOCK, CHUNK), jnp.float32),
            pltpu.SemaphoreType.DMA((len(pieces),)),
            pltpu.SemaphoreType.DMA((DEPTH,)),
            pltpu.SemaphoreType.DMA((DEPTH,)),
        ],
        out_shape=jax.ShapeDtypeStruct((width, cols), jnp.float32),
        input_output_aliases={len(pieces) + 2: 0} if aliased else {},
        compiler_params=PARAMS,
        cost_estimate=pl.CostEstimate(
            flops=2 * BLOCK * BLOCK * cols * len(blocks),
            transcendentals=0,
            bytes_accessed=6 * BLOCK * cols * len(blocks),
        ),
        name="apply",
    )(info, *pieces, grad_weight, *([result] if aliased else []))


def local_any(step, activations, grad_weight):
    groups = lax.axis_size("dp")
    layer = step[0] % LAYERS
    damping = 0.05 + 0.1 * step[0].astype(jnp.float32) / 1000.0
    tokens = activations.shape[1] * groups
    nblock = activations.shape[2] // BLOCK
    damping = damping.reshape(1)
    info = jnp.stack([layer, *[0] * 12, *range(nblock)]).astype(jnp.int32)
    (part,) = gram(info, activations, nblock, False)
    summed = lax.psum(part.astype(jnp.float32), "dp")
    each = jnp.stack([squares(summed[b], damping[0], tokens) for b in range(nblock)])
    top = jnp.broadcast_to(lax.pmax(jnp.max(each), "tensor"), (8, 128))
    result = None
    for b in range(nblock):
        p2, p3 = powers(damping, summed[b], tokens)
        inverse, _ = finish(info, damping, top, summed[b], p2, p3, tokens)
        result = apply_blocks(info, [13 + b], 12, [inverse], grad_weight, result)
    return result


def assemble_body(info, damp, *refs, count, tokens, first):
    pieces = refs[:count]
    out, total = refs[count:]
    n = ROWS // count
    for p, piece in enumerate(pieces):
        start = pl.multiple_of(info[first + p] * n, 64)
        out[pl.ds(start, n), :] = piece[...]
    total[...] = jnp.full(total.shape, squares(out[...], damp[0], tokens), jnp.float32)


def assemble(info, first, damping, pieces, tokens):
    return pl.pallas_call(
        lambda *refs: assemble_body(*refs, count=len(pieces), tokens=tokens, first=first),
        in_specs=[SM, SM] + [VM] * len(pieces),
        out_specs=[VM, VM],
        out_shape=[
            jax.ShapeDtypeStruct((ROWS, TILE), jnp.bfloat16),
            jax.ShapeDtypeStruct((8, 128), jnp.float32),
        ],
        compiler_params=PARAMS,
        name="assemble",
    )(info, damping, *pieces)


def local_quad(step, activations, grad_weight):
    groups = lax.axis_size("dp")
    halves = lax.axis_size("tensor")
    layer = step[0] % LAYERS
    damping = 0.05 + 0.1 * step[0].astype(jnp.float32) / 1000.0
    tokens = activations.shape[1] * groups
    nblock = groups // 4
    me = lax.axis_index("dp")
    z, y, c = me // 4, (me // 2) % 2, me % 2
    f32 = jnp.float32
    bf = jnp.bfloat16

    def move(v, f):
        return lax.ppermute(v, "dp", [(i, f(i)) for i in range(groups)])

    def swap_c(v):
        return move(v, lambda i: i ^ 1)

    def swap_y(v):
        return move(v, lambda i: i ^ 2)

    def shift(v, k):
        return move(v, lambda i: (i + 4 * k) % groups)

    def plus(a, b):
        return (a.astype(f32) + b.astype(f32)).astype(bf)

    def scatter(v):
        parts = [lax.dynamic_index_in_dim(v, z, 0, False).astype(f32)]
        for k in range(1, nblock):
            part = lax.dynamic_index_in_dim(v, (z + k) % nblock, 0, False)
            parts.append(shift(part, k).astype(f32))
        total = parts[0]
        for p in parts[1:]:
            total = total + p
        return total.astype(bf)

    places = [3 * c + y, 3 * c + 1 - y, 3 * c + 2]
    places += [3 * (1 - c) + y, 3 * (1 - c) + 1 - y, 3 * (1 - c) + 2]
    spread = [2 * c + y, 2 * c + 1 - y, 2 * (1 - c) + y, 2 * (1 - c) + 1 - y]
    blocks = [(z - k) % nblock for k in range(nblock)]
    info = jnp.stack([layer, c, *places, *spread, 0, *blocks]).astype(jnp.int32)
    keep, send = gram(info, activations, nblock, True)
    got = swap_c(send)
    third = ROWS // 6

    def rows_of(v, start):
        return lax.dynamic_slice_in_dim(v, start, third, 1)

    early = 2 * third
    zpart = plus(keep[:, early:], got[:, early:])
    other = (1 - y) * third
    mine = y * third
    ysend = plus(rows_of(keep, other), rows_of(got, other))
    ygot = swap_y(ysend)
    zsum = scatter(zpart)
    ypart = (rows_of(keep, mine).astype(f32) + rows_of(got, mine).astype(f32) + ygot.astype(f32)).astype(bf)
    zfull = plus(zsum, swap_y(zsum))
    ysum = scatter(ypart)
    yother = swap_y(ysum)
    own = [ysum, yother, zfull]
    theirs = [swap_c(v) for v in own]
    damping = damping.reshape(1)
    packed, top = assemble(info, 2, damping, own + theirs, tokens)

    d = 1
    while d < nblock:
        moved = move(top, lambda i: i ^ (4 * d))
        top = jnp.maximum(top, moved)
        d *= 2
    d = 1
    while d < halves:
        top = jnp.maximum(top, lax.ppermute(top, "tensor", [(i, i ^ d) for i in range(halves)]))
        d *= 2
    p2, p3 = powers(damping, packed, tokens)
    inverse, piece = finish(info, damping, top, packed, p2, p3, tokens)

    arrived = []
    for k in range(1, nblock):
        arrived.append(shift(piece, k))
    result = apply_blocks(info, [13], 12, [inverse], grad_weight, None)
    pieces = []
    for a in arrived:
        ya = swap_y(a)
        pieces += [a, ya, swap_c(a), swap_c(ya)]
    return apply_blocks(info, [13 + k for k in range(1, nblock)], 8, pieces, grad_weight, result)


def power_of_two(n):
    return n & (n - 1) == 0


def solution(mesh):
    groups, halves = mesh.shape["dp"], mesh.shape["tensor"]

    def local(step, activations, grad_weight):
        nblock = activations.shape[2] // BLOCK
        quad = groups == 4 * nblock and nblock > 1 and power_of_two(groups) and power_of_two(halves)
        return (local_quad if quad else local_any)(step, activations, grad_weight)

    in_specs = (P(), P(None, "dp", "tensor"), P(None, "tensor", "dp"))
    out_specs = P("tensor", "dp")
    return jax.shard_map(local, mesh=mesh, in_specs=in_specs, out_specs=out_specs, check_vma=False)
```

```python
import jax
import jax.numpy as jnp
from jax import lax
from jax.experimental import pallas as pl
from jax.experimental.pallas import tpu as pltpu
from jax.sharding import PartitionSpec as P


BLOCK = 1024
LAYERS = 2
TILE = 256
HALF = TILE // 2
NT = BLOCK // TILE
QUARTS = ((0, 0), (0, HALF), (HALF, HALF))
SLOT = {}
SLOT.update({(0, j): j - 1 for j in range(1, NT)})
SLOT[0, 0] = NT - 1
OFF = [(i, j) for i in range(NT) for j in range(i + 1, NT)]
for _n, _t in enumerate([t for t in OFF if t[0] > 0] + [(d, d) for d in range(1, NT - 1)]):
    SLOT[_t] = NT + _n
DIAGS = [SLOT[d, d] for d in range(NT - 1)]
ROWS = len(SLOT) * TILE
EARLY = NT * TILE
UNIT = 64
LIMIT = 60 * 1024 * 1024


def pack(dst, tile_of):
    for i, j in OFF:
        s = SLOT[i, j]
        dst[s * TILE:(s + 1) * TILE, :] = tile_of(i, j).astype(dst.dtype)
    last = tile_of(NT - 1, NT - 1).astype(dst.dtype)
    for d in range(NT - 1):
        r = DIAGS[d] * TILE
        t = tile_of(d, d).astype(dst.dtype)
        dst[r:r + HALF, :] = t[:HALF, :]
        dst[r + HALF:r + TILE, HALF:] = t[HALF:, HALF:]
        y, x = QUARTS[d]
        dst[r + HALF:r + TILE, :HALF] = last[y:y + HALF, x:x + HALF]


def unpack(src, put, dtype):
    for i, j in OFF:
        s = SLOT[i, j]
        t = src[s * TILE:(s + 1) * TILE, :].astype(dtype)
        put(i * TILE, j * TILE, t)
        put(j * TILE, i * TILE, t.T)
    for d in range(NT - 1):
        r = DIAGS[d] * TILE
        o = d * TILE
        upper = src[r:r + HALF, HALF:].astype(dtype)
        put(o, o, src[r:r + HALF, :HALF].astype(dtype))
        put(o, o + HALF, upper)
        put(o + HALF, o, upper.T)
        put(o + HALF, o + HALF, src[r + HALF:r + TILE, HALF:].astype(dtype))
        y, x = QUARTS[d]
        e = (NT - 1) * TILE
        part = src[r + HALF:r + TILE, :HALF].astype(dtype)
        put(e + y, e + x, part)
        if x != y:
            put(e + x, e + y, part.T)


def dot(a, b, dims=((1,), (0,))):
    return lax.dot_general(a, b, (dims, ((), ())), preferred_element_type=jnp.float32)


def gram_body(info, acts, keep, send, scratch, *, early, late):
    base = 0 if early else EARLY
    last = (NT - 1) * TILE

    def put(row, col, v):
        scratch[row:row + v.shape[0], col:col + v.shape[1]] = v.astype(scratch.dtype)

    panels = ([0] if early else []) + (list(range(1, NT - 1)) if late else [])
    for i in panels:
        panel = dot(acts[:, i * TILE:(i + 1) * TILE], acts[:, i * TILE:], ((0,), (0,)))
        for j in range(i + 1, NT):
            o = (j - i) * TILE
            put(SLOT[i, j] * TILE - base, 0, panel[:, o:o + TILE])
        r = DIAGS[i] * TILE - base
        put(r, 0, panel[:HALF, :TILE])
        put(r + HALF, HALF, panel[HALF:, HALF:TILE])
    if early:
        corner = acts[:, last:last + HALF]
        put(DIAGS[0] * TILE - base + HALF, 0, dot(corner, corner, ((0,), (0,))))
    if late:
        edge = dot(acts[:, last:], acts[:, last + HALF:], ((0,), (0,)))
        put(DIAGS[1] * TILE - base + HALF, 0, edge[:HALF, :])
        put(DIAGS[2] * TILE - base + HALF, 0, edge[HALF:, :])
    if send is None:
        keep[...] = scratch[...]
    else:
        rows = keep.shape[0]
        core = info[1]
        keep[...] = scratch[pl.ds(pl.multiple_of(core * rows, HALF), rows), :]
        send[...] = scratch[pl.ds(pl.multiple_of((1 - core) * rows, HALF), rows), :]


def gram(info, activations, nblock, split, early=True, late=True):
    tok = activations.shape[1]
    size = (EARLY if early else 0) + (ROWS - EARLY if late else 0)
    rows = size // 2 if split else size
    spec = pl.BlockSpec((None, rows, TILE), lambda b, info: (b, 0, 0))
    shape = jax.ShapeDtypeStruct((nblock, rows, TILE), jnp.bfloat16)

    def body(info, acts, *rest):
        if not split:
            rest = (rest[0], None, rest[1])
        gram_body(info, acts, *rest, early=early, late=late)

    return pl.pallas_call(
        body,
        grid_spec=pltpu.PrefetchScalarGridSpec(
            num_scalar_prefetch=1,
            grid=(nblock,),
            in_specs=[pl.BlockSpec((None, tok, BLOCK), lambda b, info: (info[0], 0, b))],
            out_specs=[spec, spec] if split else [spec],
            scratch_shapes=[pltpu.VMEM((size, TILE), jnp.bfloat16)],
        ),
        out_shape=[shape, shape] if split else [shape],
        compiler_params=pltpu.CompilerParams(vmem_limit_bytes=LIMIT),
        cost_estimate=pl.CostEstimate(
            flops=nblock * tok * BLOCK * BLOCK // 2, transcendentals=0, bytes_accessed=nblock * tok * BLOCK * 2
        ),
        name="gram",
    )(info, activations)


def squares(packed, damping, tokens):
    f = packed.astype(jnp.float32)
    r = lax.broadcasted_iota(jnp.int32, (ROWS, TILE), 0)
    c = lax.broadcasted_iota(jnp.int32, (ROWS, TILE), 1)
    slot = r // TILE
    rr = r % TILE
    diag = (slot == DIAGS[0]) | (slot == DIAGS[1]) | (slot == DIAGS[2])
    low = (rr >= HALF) & (c < HALF)
    mixed = slot == DIAGS[1]
    on = ((low & (rr - HALF == c) & ~mixed) | (rr == c)) & diag
    twice = ~diag | (low & mixed) | ((rr < HALF) & (c >= HALF))
    f = f / tokens + jnp.where(on, damping, 0.0)
    return jnp.sum(f * f * jnp.where(twice, 2.0, 1.0))


def factor_into(damp, packed, f, fb, tokens):
    damping = damp[0]
    inv = 1.0 / tokens

    def put(r, c, v):
        h, w = v.shape
        v = v * inv
        if r == c:
            eye = (lax.broadcasted_iota(jnp.int32, v.shape, 0)
                   == lax.broadcasted_iota(jnp.int32, v.shape, 1))
            v = v + jnp.where(eye, damping, 0.0)
        if f is not None:
            f[r:r + h, c:c + w] = v
        if fb is not None:
            fb[r:r + h, c:c + w] = v.astype(jnp.bfloat16)

    unpack(packed, put, jnp.float32)


STRIPS = [slice(i * TILE, (i + 1) * TILE) for i in range(NT)]


VM = pl.BlockSpec(memory_space=pltpu.VMEM)
SM = pl.BlockSpec(memory_space=pltpu.SMEM)
THIN = jax.ShapeDtypeStruct((BLOCK, BLOCK), jnp.bfloat16)
PARAMS = pltpu.CompilerParams(vmem_limit_bytes=LIMIT)


ANY = pl.BlockSpec(memory_space=pl.ANY)
VFULL = pltpu.VMEM((BLOCK, BLOCK), jnp.float32)
VTHIN = pltpu.VMEM((BLOCK, BLOCK), jnp.bfloat16)


def powers_body(damp, packed, h2, h3, fb, p2, p3, sems, *, tokens):
    factor_into(damp, packed, None, fb, tokens)
    for r in STRIPS:
        p2[r, :] = dot(fb[r, :], fb[...]).astype(p2.dtype)
    first = pltpu.make_async_copy(p2, h2, sems.at[0])
    first.start()
    for r in STRIPS:
        p3[r, :] = dot(p2[r, :], fb[...]).astype(p3.dtype)
    second = pltpu.make_async_copy(p3, h3, sems.at[1])
    second.start()
    first.wait()
    second.wait()


def powers(damping, packed, tokens):
    return pl.pallas_call(
        lambda *refs: powers_body(*refs, tokens=tokens),
        in_specs=[SM, VM],
        out_specs=[ANY, ANY],
        out_shape=[THIN, THIN],
        scratch_shapes=[VTHIN, VTHIN, VTHIN, pltpu.SemaphoreType.DMA((2,))],
        compiler_params=PARAMS,
        cost_estimate=pl.CostEstimate(
            flops=4 * BLOCK**3, transcendentals=0, bytes_accessed=BLOCK * BLOCK * 6
        ),
        name="powers",
    )(damping, packed)


def finish_body(info, damp, top, packed, h2, h3, out, piece, f, p2, p3, e, h, k, eb, kb, sems, *, tokens):
    loads = [pltpu.make_async_copy(a, b, sems.at[i]) for i, (a, b) in enumerate(((h2, p2), (h3, p3)))]
    for load in loads:
        load.start()
    factor_into(damp, packed, f, None, tokens)
    c = 1.0 / jnp.sqrt(jnp.max(top[...], axis=(0, 1), keepdims=True))
    for load in loads:
        load.wait()
    for r in STRIPS:
        cf = c * f[r, :]
        q2 = (c * c) * p2[r, :].astype(jnp.float32)
        q3 = (c * c * c) * p3[r, :].astype(jnp.float32)
        v = 3.0 * (cf - q2) + q3
        e[r, :] = v
        eb[r, :] = v.astype(jnp.bfloat16)
        f[r, :] = 6.0 * cf - 4.0 * q2 + q3
    for r in STRIPS:
        hv = 2.0 * e[r, :] - dot(eb[r, :], eb[...])
        h[r, :] = hv
        w = hv + 0.5 * e[r, :]
        kb[r, :] = w.astype(jnp.bfloat16)
    for r in STRIPS:
        k[r, :] = 3.75 * h[r, :] + 2.5 * e[r, :] - dot(kb[r, :], kb[...])
    for r in STRIPS:
        kb[r, :] = k[r, :].astype(jnp.bfloat16)
    for i, r in enumerate(STRIPS):
        cols = slice(i * TILE, BLOCK)
        x = dot(f[r, :].astype(jnp.bfloat16), kb[:, cols]) - 3.0 * k[r, cols] - 5.0 * f[r, cols]
        eye = (lax.broadcasted_iota(jnp.int32, x.shape, 0)
               == lax.broadcasted_iota(jnp.int32, x.shape, 1))
        e[r, cols] = c * (x + jnp.where(eye, 16.0, 0.0))
    pack(out, lambda i, j: e[i * TILE:(i + 1) * TILE, j * TILE:(j + 1) * TILE])
    n = piece.shape[0]
    piece[...] = out[pl.ds(pl.multiple_of(info[8] * n, HALF // 2), n), :]


def finish(info, damping, top, packed, p2, p3, tokens):
    return pl.pallas_call(
        lambda *refs: finish_body(*refs, tokens=tokens),
        in_specs=[SM, SM, VM, VM, ANY, ANY],
        out_specs=[VM, VM],
        out_shape=[
            jax.ShapeDtypeStruct((ROWS, TILE), jnp.bfloat16),
            jax.ShapeDtypeStruct((ROWS // 4, TILE), jnp.bfloat16),
        ],
        scratch_shapes=[VFULL, VTHIN, VTHIN, VFULL, VFULL, VFULL, VTHIN, VTHIN,
                        pltpu.SemaphoreType.DMA((2,))],
        compiler_params=PARAMS,
        name="finish",
    )(info, damping, top, packed, p2, p3)


CHUNK = 512
DEPTH = 3


def apply_body(info, *refs, count, blocks, first, aliased, cols):
    npiece = count * len(blocks)
    pieces = refs[:npiece]
    grads = refs[npiece]
    out, packed, x, g, o, psem, gsem, osem = refs[npiece + 1 + aliased:]
    n = ROWS // count
    chunks = [(c, min(CHUNK, cols - c)) for c in range(0, cols, CHUNK)]
    steps = [(b, c, w) for b in range(len(blocks)) for c, w in chunks]

    def rows(b):
        return pl.ds(pl.multiple_of(info[blocks[b]] * BLOCK, BLOCK), BLOCK)

    def load(s):
        b, c, w = steps[s]
        return pltpu.make_async_copy(
            grads.at[info[0], rows(b), pl.ds(c, w)], g.at[s % DEPTH, :, pl.ds(0, w)], gsem.at[s % DEPTH])

    def store(s):
        b, c, w = steps[s]
        return pltpu.make_async_copy(
            o.at[s % DEPTH, :, pl.ds(0, w)], out.at[rows(b), pl.ds(c, w)], osem.at[s % DEPTH])

    def fetch(b, p):
        start = pl.multiple_of(info[first + p] * n, HALF // 2)
        return pltpu.make_async_copy(
            pieces[b * count + p], packed.at[b, pl.ds(start, n), :], psem.at[b * count + p])

    for b in range(len(blocks)):
        for p in range(count):
            fetch(b, p).start()
    for s in range(min(DEPTH, len(steps))):
        load(s).start()
    for s, (b, c, w) in enumerate(steps):
        if c == 0:
            for p in range(count):
                fetch(b, p).wait()

            def put(r, col, v):
                x[b % 2, r:r + v.shape[0], col:col + v.shape[1]] = v

            unpack(packed.at[b], put, x.dtype)
        load(s).wait()
        if s >= DEPTH:
            store(s - DEPTH).wait()
        for r in STRIPS:
            o[s % DEPTH, r, :w] = dot(x[b % 2, r, :], g[s % DEPTH, :, :w])
        store(s).start()
        if s + DEPTH < len(steps):
            load(s + DEPTH).start()
    for s in range(max(0, len(steps) - DEPTH), len(steps)):
        store(s).wait()


def apply_blocks(info, blocks, first, pieces, grad_weight, result):
    width, cols = grad_weight.shape[1:]
    count = len(pieces) // len(blocks)
    aliased = result is not None
    return pl.pallas_call(
        lambda *refs: apply_body(
            *refs, count=count, blocks=blocks, first=first, aliased=int(aliased), cols=cols),
        in_specs=[SM] + [ANY] * (len(pieces) + 1 + int(aliased)),
        out_specs=ANY,
        scratch_shapes=[
            pltpu.VMEM((len(blocks), ROWS, TILE), jnp.bfloat16),
            pltpu.VMEM((2, BLOCK, BLOCK), jnp.bfloat16),
            pltpu.VMEM((DEPTH, BLOCK, CHUNK), jnp.bfloat16),
            pltpu.VMEM((DEPTH, BLOCK, CHUNK), jnp.float32),
            pltpu.SemaphoreType.DMA((len(pieces),)),
            pltpu.SemaphoreType.DMA((DEPTH,)),
            pltpu.SemaphoreType.DMA((DEPTH,)),
        ],
        out_shape=jax.ShapeDtypeStruct((width, cols), jnp.float32),
        input_output_aliases={len(pieces) + 2: 0} if aliased else {},
        compiler_params=PARAMS,
        cost_estimate=pl.CostEstimate(
            flops=2 * BLOCK * BLOCK * cols * len(blocks),
            transcendentals=0,
            bytes_accessed=6 * BLOCK * cols * len(blocks),
        ),
        name="apply",
    )(info, *pieces, grad_weight, *([result] if aliased else []))


def local_any(step, activations, grad_weight):
    groups = lax.axis_size("dp")
    layer = step[0] % LAYERS
    damping = 0.05 + 0.1 * step[0].astype(jnp.float32) / 1000.0
    tokens = activations.shape[1] * groups
    nblock = activations.shape[2] // BLOCK
    damping = damping.reshape(1)
    info = jnp.stack([layer, *[0] * 12, *range(nblock)]).astype(jnp.int32)
    (part,) = gram(info, activations, nblock, False)
    summed = lax.psum(part.astype(jnp.float32), "dp")
    each = jnp.stack([squares(summed[b], damping[0], tokens) for b in range(nblock)])
    top = jnp.broadcast_to(lax.pmax(jnp.max(each), "tensor"), (8, 128))
    result = None
    for b in range(nblock):
        p2, p3 = powers(damping, summed[b], tokens)
        inverse, _ = finish(info, damping, top, summed[b], p2, p3, tokens)
        result = apply_blocks(info, [13 + b], 12, [inverse], grad_weight, result)
    return result


def assemble_body(info, damp, *refs, count, tokens, first):
    pieces = refs[:count]
    out, total = refs[count:]
    for p, piece in enumerate(pieces):
        start = pl.multiple_of(info[first + p] * UNIT, UNIT)
        out[pl.ds(start, piece.shape[0]), :] = piece[...]
    total[...] = jnp.full(total.shape, squares(out[...], damp[0], tokens), jnp.float32)


def assemble(info, first, damping, pieces, tokens):
    return pl.pallas_call(
        lambda *refs: assemble_body(*refs, count=len(pieces), tokens=tokens, first=first),
        in_specs=[SM, SM] + [VM] * len(pieces),
        out_specs=[VM, VM],
        out_shape=[
            jax.ShapeDtypeStruct((ROWS, TILE), jnp.bfloat16),
            jax.ShapeDtypeStruct((8, 128), jnp.float32),
        ],
        compiler_params=PARAMS,
        name="assemble",
    )(info, damping, *pieces)


def local_quad(step, activations, grad_weight):
    groups = lax.axis_size("dp")
    halves = lax.axis_size("tensor")
    layer = step[0] % LAYERS
    damping = 0.05 + 0.1 * step[0].astype(jnp.float32) / 1000.0
    tokens = activations.shape[1] * groups
    nblock = groups // 4
    me = lax.axis_index("dp")
    z, y, c = me // 4, (me // 2) % 2, me % 2
    f32 = jnp.float32
    bf = jnp.bfloat16

    def move(v, f):
        return lax.ppermute(v, "dp", [(i, f(i)) for i in range(groups)])

    def swap_c(v):
        return move(v, lambda i: i ^ 1)

    def swap_y(v):
        return move(v, lambda i: i ^ 2)

    def shift(v, k):
        return move(v, lambda i: (i + 4 * k) % groups)

    def plus(a, b):
        return (a.astype(f32) + b.astype(f32)).astype(bf)

    def scatter(v):
        parts = [lax.dynamic_index_in_dim(v, z, 0, False).astype(f32)]
        for k in range(1, nblock):
            part = lax.dynamic_index_in_dim(v, (z + k) % nblock, 0, False)
            parts.append(shift(part, k).astype(f32))
        total = parts[0]
        for p in parts[1:]:
            total = total + p
        return total.astype(bf)

    third = ROWS // 6

    def places_of(core):
        start = 3 * core * third
        return [(start + n * third) // UNIT for n in (y, 1 - y, 2)]

    places = places_of(c) + places_of(1 - c)
    spread = [2 * c + y, 2 * c + 1 - y, 2 * (1 - c) + y, 2 * (1 - c) + 1 - y]
    blocks = [(z - k) % nblock for k in range(nblock)]
    info = jnp.stack([layer, c, *places, *spread, 0, *blocks]).astype(jnp.int32)
    keep, send = gram(info, activations, nblock, True)
    got = swap_c(send)

    def rows_of(v, start):
        return lax.dynamic_slice_in_dim(v, start, third, 1)

    zpart = plus(keep[:, 2 * third:], got[:, 2 * third:])
    other = (1 - y) * third
    mine = y * third
    ysend = plus(rows_of(keep, other), rows_of(got, other))
    ygot = swap_y(ysend)
    zsum = scatter(zpart)
    ypart = (rows_of(keep, mine).astype(f32) + rows_of(got, mine).astype(f32) + ygot.astype(f32)).astype(bf)
    zfull = plus(zsum, swap_y(zsum))
    ysum = scatter(ypart)
    yother = swap_y(ysum)
    own = [ysum, yother, zfull]
    theirs = [swap_c(v) for v in own]
    damping = damping.reshape(1)
    packed, top = assemble(info, 2, damping, own + theirs, tokens)

    tops = [top]
    for k in range(1, nblock):
        tops.append(shift(top, k))
    for other in tops[1:]:
        top = jnp.maximum(top, other)
    d = 1
    while d < halves:
        top = jnp.maximum(top, lax.ppermute(top, "tensor", [(i, i ^ d) for i in range(halves)]))
        d *= 2
    p2, p3 = powers(damping, packed, tokens)
    inverse, piece = finish(info, damping, top, packed, p2, p3, tokens)

    arrived = []
    for k in range(1, nblock):
        arrived.append(shift(arrived[0], 1) if k == 2 and nblock == 4 else shift(piece, k))
    result = apply_blocks(info, [13], 12, [inverse], grad_weight, None)
    pieces = []
    for k, a in zip(range(1, nblock), arrived):
        ya = swap_y(a)
        pieces.append([a, ya, swap_c(a), swap_c(ya)])
    result = apply_blocks(info, [12 + nblock], 8, pieces[-1], grad_weight, result)
    rest = [p for four in pieces[:-1] for p in four]
    return apply_blocks(info, [13 + k for k in range(1, nblock - 1)], 8, rest, grad_weight, result)


def power_of_two(n):
    return n & (n - 1) == 0


def solution(mesh):
    groups, halves = mesh.shape["dp"], mesh.shape["tensor"]

    def local(step, activations, grad_weight):
        nblock = activations.shape[2] // BLOCK
        quad = groups == 4 * nblock and nblock > 2 and power_of_two(groups) and power_of_two(halves)
        return (local_quad if quad else local_any)(step, activations, grad_weight)

    in_specs = (P(), P(None, "dp", "tensor"), P(None, "tensor", "dp"))
    out_specs = P("tensor", "dp")
    return jax.shard_map(local, mesh=mesh, in_specs=in_specs, out_specs=out_specs, check_vma=False)
```
